32 devices in a mesh: groups: 2 (over x), seq: 16 (over z, y, core).
Axes of the slice: x: 2, y: 2, z: 4, core: 2. Of those that a mesh axis runs over, the one named last changes fastest.
Arguments:
- self_query: bfloat16 [16, 8192], P('groups'), parts along dimension 0, may hold values from -128 to 128
- new_key: bfloat16 [16, 8192], P('groups'), parts along dimension 0, may hold values from -6 to 6
- new_value: bfloat16 [16, 8192], P('groups'), parts along dimension 0, may hold values from -12 to 12
- cache_keys: bfloat16 [16, 1024, 8192], P('groups', 'seq'), parts along dimension 0, may hold values from -8 to 8
- cache_values: bfloat16 [16, 1024, 8192], P('groups', 'seq'), parts along dimension 0, may hold values from -12 to 12
- lengths: int32 [16], P('groups'), parts along dimension 0, may hold values from 128 to 1024
- db_keys: bfloat16 [32, 128, 8192], P(('groups', 'seq')), parts along dimension 0, may hold values from -8 to 8
- db_values: bfloat16 [32, 128, 8192], P(('groups', 'seq')), parts along dimension 0, may hold values from -12 to 12
- cross_query: bfloat16 [16, 8192], P('groups'), parts along dimension 0, may hold values from -128 to 128
- neighbour_ids: int32 [16, 2], P('groups'), parts along dimension 0, may hold values from 0 to 15
Outputs:
- self_out: bfloat16 [16, 8192], P('groups', 'seq'), parts along dimension 0
- cross_out: bfloat16 [16, 8192], P('groups', 'seq'), parts along dimension 0
The draws below stay inside these ranges and needn't reach their ends.
There are 2 independent parts, one for each index of `groups`. The reference program is written for one: setup_inputs(seed, part) draws one part's arguments, and reference() takes and returns one part's arrays. A program takes and returns all parts, laid end to end along the dimension named above; each array names one. Nothing has to cross between parts.
Inputs may be any that keep to these rules, and one draw needn't show every extreme that they name: `neighbour_ids`: the 2 ids of a row may repeat.
All inputs are finite; a program needn't handle non-finite values.
Results may differ from the reference program's by a relative error of at most 0.022.
Values may be sent and summed in bfloat16 or wider, within the bound.
A program may use at most 64 MiB of HBM per device.

```python
import jax
import jax.numpy as jnp
from jax import lax

H = 64
DH = 128
HD = 8192
ROWS = 8
L = 1024
NBR = 2
NTOK = 128
NDB = 16


def draw_cache_keys(key, part):
    keys = jax.random.normal(jax.random.fold_in(key, 11), (ROWS, L, HD), jnp.float32)
    return keys.astype(jnp.bfloat16)


def draw_self_query(key, part):
    query = 1.5 * jax.random.normal(jax.random.fold_in(key, 12), (ROWS, HD), jnp.float32)
    return query.astype(jnp.bfloat16)


def draw_db_keys(key, part):
    keys = jax.random.normal(jax.random.fold_in(key, 13), (NDB, NTOK, HD), jnp.float32)
    return keys.astype(jnp.bfloat16)


def draw_cross_query(key, part):
    query = 1.5 * jax.random.normal(jax.random.fold_in(key, 14), (ROWS, HD), jnp.float32)
    return query.astype(jnp.bfloat16)


def place_ends(result, own_key, smallest, largest):
    longest = result.shape.index(max(result.shape))
    spots = []
    for shift in (0, 1):
        where = [jax.random.randint(jax.random.fold_in(own_key, axis), (), 0, length) for axis, length in enumerate(result.shape)]
        where[longest] = (where[longest] + shift) % result.shape[longest]
        spots.append(tuple(where))
    return result.at[spots[0]].set(smallest).at[spots[1]].set(largest)


def block_scale(stream_key, extent, pieces, smallest, top_value):
    def one(position, blocks):
        draws = jax.random.uniform(jax.random.fold_in(jax.random.fold_in(stream_key, 6), position), (blocks,), jnp.float32, smallest / len(pieces), top_value / len(pieces))
        return jnp.repeat(jnp.exp(draws), extent[position] // blocks).reshape((-1,) + (1,) * (len(extent) - position - 1))

    level = one(*pieces[0])
    for cut in pieces[1:]:
        level = level * one(*cut)
    return level


def normal_values(key, dims, width, most, shards=(), held_as=jnp.bfloat16):
    level = block_scale(key, dims, shards, -0.22, 0.18) if shards else 1.0
    array = jax.random.normal(key, dims, jnp.float32) * width * level
    return jnp.minimum(jnp.maximum(array, -most), most).astype(held_as)


def setup_inputs(seed: int = 0, part: int = 0) -> dict:
    splits = jax.random.split(jax.random.key(seed), 11)
    part_keys = jax.random.split(jax.random.fold_in(splits[10], part), 11)
    return {
        "self_query": draw_self_query(jax.random.fold_in(jax.random.fold_in(splits[10], part), 71), part),
        "new_key": normal_values(part_keys[1], (ROWS, HD), 1.0, 6.0),
        "new_value": normal_values(part_keys[2], (ROWS, HD), 3.0, 12.0),
        "cache_keys": draw_cache_keys(jax.random.fold_in(jax.random.fold_in(splits[10], part), 71), part),
        "cache_values": normal_values(part_keys[4], (ROWS, L, HD), 3.0, 12.0, ((1, 16),)),
        "lengths": place_ends(jax.random.randint(part_keys[5], (ROWS,), max(16, L // 8), L + 1), jax.random.fold_in(part_keys[5], 1), max(16, L // 8), L).astype(jnp.int32),
        "db_keys": draw_db_keys(jax.random.fold_in(jax.random.fold_in(splits[10], part), 71), part),
        "db_values": normal_values(part_keys[7], (NDB, NTOK, HD), 3.0, 12.0, ((0, 16),)),
        "cross_query": draw_cross_query(jax.random.fold_in(jax.random.fold_in(splits[10], part), 71), part),
        "neighbour_ids": place_ends(jax.random.randint(part_keys[9], (ROWS, NBR), 0, NDB), jax.random.fold_in(part_keys[9], 1), 0, NDB - 1).astype(jnp.int32),
    }


NEG = -1e30


def self_row(args):
    query, keys, values, key_new, value_new, length = args
    scale = DH ** -0.5
    q = query.astype(jnp.float32).reshape(H, DH)
    k = keys.astype(jnp.float32).reshape(L, H, DH)
    s = jnp.einsum('hd,phd->hp', q, k) * scale
    live = jnp.arange(L, dtype=jnp.int32)[None, :] < length
    s = jnp.where(live, s, NEG)
    s_own = jnp.sum(q * key_new.astype(jnp.float32).reshape(H, DH), axis=1) * scale
    peak = jnp.maximum(jnp.max(s, axis=1), s_own)
    e = jnp.where(live, jnp.exp(s - peak[:, None]), 0.0)
    e_own = jnp.exp(s_own - peak)
    den = jnp.sum(e, axis=1) + e_own
    w = e.astype(jnp.bfloat16).astype(jnp.float32)
    w_own = e_own.astype(jnp.bfloat16).astype(jnp.float32)
    v = values.astype(jnp.float32).reshape(L, H, DH)
    num = jnp.einsum('hp,phd->hd', w, v) + w_own[:, None] * value_new.astype(jnp.float32).reshape(H, DH)
    return (num / den[:, None]).reshape(HD).astype(jnp.bfloat16)


def cross_row(args):
    query, ids, db_keys, db_values = args
    scale = DH ** -0.5
    q = query.astype(jnp.float32).reshape(H, DH)
    k = jnp.take(db_keys, ids, axis=0).astype(jnp.float32).reshape(NBR * NTOK, H, DH)
    v = jnp.take(db_values, ids, axis=0).astype(jnp.float32).reshape(NBR * NTOK, H, DH)
    s = jnp.einsum('hd,thd->ht', q, k) * scale
    peak = jnp.max(s, axis=1)
    e = jnp.exp(s - peak[:, None])
    den = jnp.sum(e, axis=1)
    w = e.astype(jnp.bfloat16).astype(jnp.float32)
    num = jnp.einsum('ht,thd->hd', w, v)
    return (num / den[:, None]).reshape(HD).astype(jnp.bfloat16)


def reference(self_query, new_key, new_value, cache_keys, cache_values, lengths, db_keys, db_values, cross_query, neighbour_ids):
    self_out = lax.map(self_row, (self_query, cache_keys, cache_values, new_key, new_value, lengths.astype(jnp.int32)))
    cross_out = lax.map(lambda a: cross_row((a[0], a[1], db_keys, db_values)), (cross_query, neighbour_ids.astype(jnp.int32)))
    return self_out, cross_out
```

```python
import functools

import jax
import jax.numpy as jnp
from jax import lax
from jax.experimental import pallas as pl
from jax.experimental.pallas import tpu as pltpu
from jax.sharding import PartitionSpec as P

DH = 128
NEG = -1e30
FLOOR = -1e29
MESH = pl.DeviceIdType.MESH


def offset_of(step, count):
    return count // 2 + ((step + 1) // 2) * (1 - 2 * (step % 2))


def pair_queries(block):
    rows = block.shape[0]
    both = jnp.concatenate([block, block], axis=0)
    row = lax.broadcasted_iota(jnp.int32, both.shape, 0)
    lane = lax.broadcasted_iota(jnp.int32, both.shape, 1)
    return jnp.where((row < rows) == (lane < DH), both, 0.0).astype(jnp.bfloat16)


def attend(query, keys, values, bias, counts):
    scores = lax.dot_general(
        query, keys, (((1,), (1,)), ((), ())), preferred_element_type=jnp.float32
    )
    scores = scores * (DH ** (-0.5)) + bias
    peak = jnp.maximum(jnp.max(scores, axis=1, keepdims=True), FLOOR)
    weights = jnp.exp(scores - peak)
    if counts is not None:
        weights = weights * counts
    den = jnp.maximum(jnp.sum(weights, axis=1, keepdims=True), 0.5)
    acc = jnp.dot(weights.astype(jnp.bfloat16), values, preferred_element_type=jnp.float32)
    return peak + jnp.log(den), acc * (1.0 / den)


def kernel(
    parts,
    group,
    lengths,
    ids,
    self_query,
    new_key,
    new_value,
    cache_keys,
    cache_values,
    db_keys,
    db_values,
    cross_query,
    self_out,
    cross_out,
    keys,
    values,
    dkeys,
    dvalues,
    squery,
    cquery,
    nkey,
    nvalue,
    bias,
    cbias,
    ccounts,
    outbox,
    inbox,
    stats,
    stream_sem,
    small_sem,
    send_sem,
    recv_sem,
):
    me = lax.axis_index("seq")
    rows, positions, width = cache_keys.shape
    entries, tokens, _ = db_keys.shape
    span = width // parts
    pairs = span // (2 * DH)
    columns = 2 * pairs

    def target(step):
        return lax.rem(me + offset_of(step, parts), parts)

    def lanes_of(device):
        return pl.ds(pl.multiple_of(device * span, span), span)

    def streams(step):
        lanes = lanes_of(target(step))
        return [
            pltpu.make_async_copy(source.at[:, :, lanes], dest.at[step], stream_sem.at[k, step])
            for k, (source, dest) in enumerate(
                (
                    (cache_keys, keys),
                    (cache_values, values),
                    (db_keys, dkeys),
                    (db_values, dvalues),
                )
            )
        ]

    def message(step):
        return pltpu.make_async_remote_copy(
            src_ref=outbox.at[step],
            dst_ref=inbox.at[step],
            send_sem=send_sem.at[step],
            recv_sem=recv_sem.at[step],
            device_id={"seq": target(step)},
            device_id_type=MESH,
        )

    own = lanes_of(me)
    small = [
        pltpu.make_async_copy(self_query, squery, small_sem.at[0]),
        pltpu.make_async_copy(cross_query, cquery, small_sem.at[1]),
        pltpu.make_async_copy(new_key.at[:, own], nkey, small_sem.at[2]),
        pltpu.make_async_copy(new_value.at[:, own], nvalue, small_sem.at[3]),
    ]
    small[0].start()
    small[1].start()

    def launch(step, carry):
        for copy in streams(step):
            copy.start()
        return carry

    lax.fori_loop(0, parts, launch, 0)
    small[2].start()
    small[3].start()

    barrier = pltpu.get_barrier_semaphore()

    def greet(step, carry):
        pl.semaphore_signal(
            barrier, inc=1, device_id={"seq": target(step)}, device_id_type=MESH
        )
        return carry

    lax.fori_loop(0, parts - 1, greet, 0)

    shape = (2 * rows, rows * positions)
    row = lax.broadcasted_iota(jnp.int32, shape, 0)
    row = jnp.where(row >= rows, row - rows, row)
    lane = lax.broadcasted_iota(jnp.int32, shape, 1)
    table = jnp.full(shape, NEG, jnp.float32)
    for b in range(rows):
        left = jnp.clip(lengths[b] - me * positions, 0, positions)
        live = (row == b) & (lane >= b * positions) & (lane < b * positions + left)
        table = jnp.where(live, 0.0, table)
    bias[...] = table
    shape = (2 * rows, entries * tokens)
    row = lax.broadcasted_iota(jnp.int32, shape, 0)
    row = jnp.where(row >= rows, row - rows, row)
    lane = lax.broadcasted_iota(jnp.int32, shape, 1)
    table = jnp.zeros(shape, jnp.float32)
    for b in range(rows):
        for e in range(entries):
            here = (row == b) & (lane >= e * tokens) & (lane < (e + 1) * tokens)
            for j in range(ids.shape[1]):
                match = here & (jnp.full(shape, ids[b, j], jnp.int32) == me * entries + e)
                table = jnp.where(match, table + 1.0, table)
    ccounts[...] = table
    cbias[...] = jnp.where(table > 0.0, 0.0, NEG)

    small[0].wait()
    small[1].wait()
    tag = lax.broadcasted_iota(jnp.int32, (2 * rows, DH), 1)

    def compute(step):
        device = target(step)
        found = [None] * columns
        sums = []
        for pair in range(pairs):
            lanes = pl.ds(pl.multiple_of(device * span, span) + pair * 2 * DH, 2 * DH)
            piece = slice(pair * 2 * DH, (pair + 1) * 2 * DH)
            found[pair], acc = attend(
                pair_queries(squery[:, lanes].astype(jnp.float32)),
                keys[step, :, :, piece].reshape(rows * positions, 2 * DH),
                values[step, :, :, piece].reshape(rows * positions, 2 * DH),
                bias[...],
                None,
            )
            found[pairs + pair], cacc = attend(
                pair_queries(cquery[:, lanes].astype(jnp.float32)),
                dkeys[step, :, :, piece].reshape(entries * tokens, 2 * DH),
                dvalues[step, :, :, piece].reshape(entries * tokens, 2 * DH),
                cbias[...],
                ccounts[...],
            )
            sums.append(jnp.concatenate([acc[:rows, :DH], cacc[:rows, :DH]], axis=0))
            sums.append(jnp.concatenate([acc[rows:, DH:], cacc[rows:, DH:]], axis=0))
        for head, part in enumerate(sums):
            outbox[step, :, head * DH : (head + 1) * DH] = part.astype(jnp.bfloat16)
        level = jnp.zeros((2 * rows, DH), jnp.float32)
        for k in range(3 * columns):
            level = jnp.where(tag == k, found[k % columns], level)
        high = level.astype(jnp.bfloat16).astype(jnp.float32)
        rest = level - high
        middle = rest.astype(jnp.bfloat16).astype(jnp.float32)
        low = rest - middle
        level = jnp.where(tag < columns, high, jnp.where(tag < 2 * columns, middle, low))
        outbox[step, :, span:] = level.astype(jnp.bfloat16)

    def block(first, count, wait_barrier, sends):
        for j in range(count):
            for copy in streams(first + j):
                copy.wait()
        for j in range(count):
            compute(first + j)
        if wait_barrier:
            pl.semaphore_wait(barrier, parts - 1)
        for j in range(sends):
            message(first + j).start()

    block(0, group, True, group)

    def turn(k, carry):
        block(k * group, group, False, group)
        return carry

    lax.fori_loop(1, parts // group - 1, turn, 0)
    block(parts - group, group, False, group - 1)

    small[2].wait()
    small[3].wait()
    query_own = squery[:, own].astype(jnp.float32)
    product = query_own * nkey[...].astype(jnp.float32)
    level_own = jnp.full((2 * rows, DH), NEG, jnp.float32)
    for pair in range(pairs):
        halves = [
            jnp.sum(product[:, h * DH : (h + 1) * DH], axis=1, keepdims=True) * (DH ** (-0.5))
            for h in (2 * pair, 2 * pair + 1)
        ]
        level_own = jnp.where(tag == pair, jnp.concatenate(halves, axis=0), level_own)

    def spread(tile, head):
        pair, half = head // 2, head % 2
        part = tile[half * rows : (half + 1) * rows]
        return jnp.concatenate(
            [
                jnp.broadcast_to(part[:, pair : pair + 1], (rows, DH)),
                jnp.broadcast_to(part[:, pairs + pair : pairs + pair + 1], (rows, DH)),
            ],
            axis=0,
        )

    def level_of(box, step):
        raw = box[step, :, span:].astype(jnp.float32)
        full = raw + pltpu.roll(raw, DH - columns, 1) + pltpu.roll(raw, DH - 2 * columns, 1)
        return jnp.where(tag < columns, full, NEG)

    level = level_of(outbox, parts - 1)
    stats[parts - 1] = level
    top = jnp.maximum(level_own, level)
    for step in range(parts - 1):
        message(step).wait_recv()
        level = level_of(inbox, step)
        stats[step] = level
        top = jnp.maximum(top, level)
    share = jnp.exp(level_own - top)
    total = share
    zero = jnp.zeros((rows, DH), jnp.float32)
    sums = [
        jnp.concatenate([nvalue[:, h * DH : (h + 1) * DH].astype(jnp.float32), zero], axis=0)
        * spread(share, h)
        for h in range(2 * pairs)
    ]
    for step in range(parts):
        box = inbox if step < parts - 1 else outbox
        share = jnp.exp(stats[step] - top)
        total = total + share
        for h in range(2 * pairs):
            part = box[step, :, h * DH : (h + 1) * DH].astype(jnp.float32)
            sums[h] = sums[h] + part * spread(share, h)
    inverse = 1.0 / total
    for h in range(2 * pairs):
        result = sums[h] * spread(inverse, h)
        self_out[:, h * DH : (h + 1) * DH] = result[:rows].astype(jnp.bfloat16)
        cross_out[:, h * DH : (h + 1) * DH] = result[rows:].astype(jnp.bfloat16)

    def drain(step, carry):
        message(step).wait_send()
        return carry

    lax.fori_loop(0, parts - 1, drain, 0)


def on_device(
    self_query,
    new_key,
    new_value,
    cache_keys,
    cache_values,
    lengths,
    db_keys,
    db_values,
    cross_query,
    neighbour_ids,
):
    parts = lax.axis_size("seq")
    rows, positions, width = cache_keys.shape
    entries, tokens, _ = db_keys.shape
    span = width // parts
    group = max(1, 2048 // span)
    half = jnp.bfloat16
    anywhere = pl.BlockSpec(memory_space=pl.ANY)
    scalar = pl.BlockSpec(memory_space=pltpu.SMEM)
    vmem = pl.BlockSpec(memory_space=pltpu.VMEM)
    out = jax.ShapeDtypeStruct((rows, span), half)
    return pl.pallas_call(
        functools.partial(kernel, parts, group),
        out_shape=(out, out),
        in_specs=[scalar, scalar] + [anywhere] * 8,
        out_specs=(vmem, vmem),
        scratch_shapes=[
            pltpu.VMEM((parts, rows, positions, span), half),
            pltpu.VMEM((parts, rows, positions, span), half),
            pltpu.VMEM((parts, entries, tokens, span), half),
            pltpu.VMEM((parts, entries, tokens, span), half),
            pltpu.VMEM((rows, width), half),
            pltpu.VMEM((rows, width), half),
            pltpu.VMEM((rows, span), half),
            pltpu.VMEM((rows, span), half),
            pltpu.VMEM((2 * rows, rows * positions), jnp.float32),
            pltpu.VMEM((2 * rows, entries * tokens), jnp.float32),
            pltpu.VMEM((2 * rows, entries * tokens), jnp.float32),
            pltpu.VMEM((parts, 2 * rows, span + DH), half),
            pltpu.VMEM((parts, 2 * rows, span + DH), half),
            pltpu.VMEM((parts, 2 * rows, DH), jnp.float32),
            pltpu.SemaphoreType.DMA((4, parts)),
            pltpu.SemaphoreType.DMA((4,)),
            pltpu.SemaphoreType.DMA((parts,)),
            pltpu.SemaphoreType.DMA((parts,)),
        ],
        compiler_params=pltpu.CompilerParams(
            collective_id=0, has_side_effects=True, vmem_limit_bytes=60 * 1024 * 1024
        ),
    )(
        lengths,
        neighbour_ids,
        self_query,
        new_key,
        new_value,
        cache_keys,
        cache_values,
        db_keys,
        db_values,
        cross_query,
    )


def solution(mesh):
    in_specs = (
        P("groups", None),
        P("groups", None),
        P("groups", None),
        P("groups", "seq", None),
        P("groups", "seq", None),
        P("groups"),
        P(("groups", "seq"), None, None),
        P(("groups", "seq"), None, None),
        P("groups", None),
        P("groups", None),
    )
    out_specs = (P("groups", "seq"), P("groups", "seq"))
    return jax.shard_map(
        on_device, mesh=mesh, in_specs=in_specs, out_specs=out_specs, check_vma=False
    )
```

```python
import functools

import jax
import jax.numpy as jnp
from jax import lax
from jax.experimental import pallas as pl
from jax.experimental.pallas import tpu as pltpu
from jax.sharding import PartitionSpec as P

DH = 128
NEG = -1e30
FLOOR = -1e29
MESH = pl.DeviceIdType.MESH


def offset_of(step, count):
    return count // 2 + ((step + 1) // 2) * (1 - 2 * (step % 2))


def spread_queries(block, first, total):
    rows, width = block.shape
    zero = jnp.zeros((rows, DH), block.dtype)
    heads = width // DH
    return jnp.concatenate(
        [
            jnp.concatenate(
                [
                    block[:, h * DH : (h + 1) * DH] if first + h == i else zero
                    for h in range(heads)
                ],
                axis=1,
            )
            for i in range(total)
        ],
        axis=0,
    ).astype(jnp.bfloat16)


def weigh(queries, keys, bias, counts):
    scores = sum(
        lax.dot_general(k, q, (((1,), (1,)), ((), ())), preferred_element_type=jnp.float32)
        for q, k in zip(queries, keys)
    )
    scores = scores.T * (DH ** (-0.5)) + jnp.concatenate([bias] * (scores.shape[1] // bias.shape[0]))
    peak = jnp.maximum(jnp.max(scores, axis=1, keepdims=True), FLOOR)
    weights = jnp.exp(scores - peak)
    if counts is not None:
        weights = weights * jnp.concatenate([counts] * (scores.shape[0] // counts.shape[0]))
    den = jnp.maximum(jnp.sum(weights, axis=1, keepdims=True), 0.5)
    return weights.astype(jnp.bfloat16), 1.0 / den, peak + jnp.log(den)


def kernel(
    parts,
    ahead,
    lengths_in,
    ids_in,
    self_query,
    new_key,
    new_value,
    cache_keys,
    cache_values,
    db_keys,
    db_values,
    cross_query,
    out,
    lengths,
    ids,
    keys,
    values,
    dkeys,
    dvalues,
    squery,
    cquery,
    nkey,
    nvalue,
    bias,
    cbias,
    ccounts,
    outbox,
    sidebox,
    merged,
    inbox,
    stats,
    stream_sem,
    small_sem,
    send_sem,
    recv_sem,
    side_send,
    side_recv,
):
    me = lax.axis_index("seq")
    rows, positions, width = cache_keys.shape
    entries, tokens, _ = db_keys.shape
    span = width // parts
    pairs = span // (2 * DH)
    columns = 2 * pairs

    chips = parts // 2
    core = lax.rem(me, 2)
    chip = me // 2
    partner = chip * 2 + 1 - core

    def peer(step):
        return lax.rem(chip + offset_of(step, chips), chips) * 2 + core

    def target(k):
        flip = 1 - lax.rem(k, 2)
        return peer(k // 2) - core + core * (1 - flip) + (1 - core) * flip

    def lanes_of(device):
        return pl.ds(pl.multiple_of(device * span, span), span)

    def streams(step):
        lanes = lanes_of(target(step))
        return [
            pltpu.make_async_copy(source.at[:, :, lanes], dest.at[step], stream_sem.at[k, step])
            for k, (source, dest) in enumerate(
                (
                    (cache_keys, keys),
                    (cache_values, values),
                    (db_keys, dkeys),
                    (db_values, dvalues),
                )
            )
        ]

    def handover(step):
        return pltpu.make_async_remote_copy(
            src_ref=outbox.at[2 * step],
            dst_ref=sidebox.at[step],
            send_sem=side_send.at[step],
            recv_sem=side_recv.at[step],
            device_id={"seq": partner},
            device_id_type=MESH,
        )

    def message(step):
        return pltpu.make_async_remote_copy(
            src_ref=merged.at[step],
            dst_ref=inbox.at[step],
            send_sem=send_sem.at[step],
            recv_sem=recv_sem.at[step],
            device_id={"seq": peer(step)},
            device_id_type=MESH,
        )

    own = lanes_of(me)
    small = [
        pltpu.make_async_copy(self_query, squery, small_sem.at[0]),
        pltpu.make_async_copy(cross_query, cquery, small_sem.at[1]),
        pltpu.make_async_copy(new_key.at[:, own], nkey, small_sem.at[2]),
        pltpu.make_async_copy(new_value.at[:, own], nvalue, small_sem.at[3]),
    ]
    scalars = [
        pltpu.make_async_copy(lengths_in, lengths, small_sem.at[4]),
        pltpu.make_async_copy(ids_in, ids, small_sem.at[5]),
    ]
    for copy in small[:2] + scalars:
        copy.start()

    def launch(step, carry):
        for copy in streams(step):
            copy.start()
        return carry

    lax.fori_loop(0, 2 * ahead, launch, 0)
    small[2].start()
    small[3].start()

    barrier = pltpu.get_barrier_semaphore()

    def greet(step, carry):
        pl.semaphore_signal(
            barrier, inc=1, device_id={"seq": peer(step)}, device_id_type=MESH
        )
        return carry

    lax.fori_loop(0, chips - 1, greet, 0)
    pl.semaphore_signal(barrier, inc=1, device_id={"seq": partner}, device_id_type=MESH)

    for copy in scalars:
        copy.wait()
    shape = (2 * rows, rows * positions)
    row = lax.broadcasted_iota(jnp.int32, shape, 0)
    row = jnp.where(row >= rows, row - rows, row)
    lane = lax.broadcasted_iota(jnp.int32, shape, 1)
    table = jnp.full(shape, NEG, jnp.float32)
    for b in range(rows):
        left = jnp.clip(lengths[b] - me * positions, 0, positions)
        live = (row == b) & (lane >= b * positions) & (lane < b * positions + left)
        table = jnp.where(live, 0.0, table)
    bias[...] = table
    shape = (2 * rows, entries * tokens)
    row = lax.broadcasted_iota(jnp.int32, shape, 0)
    row = jnp.where(row >= rows, row - rows, row)
    lane = lax.broadcasted_iota(jnp.int32, shape, 1)
    table = jnp.zeros(shape, jnp.float32)
    for b in range(rows):
        for e in range(entries):
            here = (row == b) & (lane >= e * tokens) & (lane < (e + 1) * tokens)
            for j in range(ids.shape[0]):
                match = here & (jnp.full(shape, ids[j, b], jnp.int32) == me * entries + e)
                table = jnp.where(match, table + 1.0, table)
    ccounts[...] = table
    cbias[...] = jnp.where(table > 0.0, 0.0, NEG)

    small[0].wait()
    small[1].wait()
    tag = lax.broadcasted_iota(jnp.int32, (2 * rows, DH), 1)

    def compute_both(first):
        heads = 2 * pairs
        results = []
        for source, held, extent, table, number in (
            (squery, keys, rows * positions, bias[...], None),
            (cquery, dkeys, entries * tokens, cbias[...], ccounts[...]),
        ):
            queries, blocks = [], []
            for j in range(2):
                lanes = lanes_of(target(first + j))
                block = source[:, lanes].astype(jnp.float32)
                queries.append(spread_queries(block, j * heads, 2 * heads))
                blocks.append(held[first + j].reshape(extent, span))
            results.append(weigh(queries, blocks, table, number))
        for j in range(2):
            compute(first + j, j, results)

    def compute(step, place, results):
        found = [None] * columns
        sums = []
        for pair in range(pairs):
            piece = slice(pair * 2 * DH, (pair + 1) * 2 * DH)
            at = slice((place * pairs + pair) * 2 * rows, (place * pairs + pair + 1) * 2 * rows)
            accs = []
            for kind, (held, extent) in enumerate(
                ((values, rows * positions), (dvalues, entries * tokens))
            ):
                weights, inverse, level = results[kind]
                acc = jnp.dot(
                    weights[at],
                    held[step, :, :, piece].reshape(extent, 2 * DH),
                    preferred_element_type=jnp.float32,
                )
                accs.append(acc * inverse[at])
                found[kind * pairs + pair] = level[at]
            acc, cacc = accs
            sums.append(jnp.concatenate([acc[:rows, :DH], cacc[:rows, :DH]], axis=0))
            sums.append(jnp.concatenate([acc[rows:, DH:], cacc[rows:, DH:]], axis=0))
        for head, part in enumerate(sums):
            outbox[step, :, head * DH : (head + 1) * DH] = part.astype(jnp.bfloat16)
        level = jnp.zeros((2 * rows, DH), jnp.float32)
        for k in range(3 * columns):
            level = jnp.where(tag == k, found[k % columns], level)
        outbox[step, :, span:] = packed(level)

    def spread(tile, head):
        pair, half = head // 2, head % 2
        part = tile[half * rows : (half + 1) * rows]
        return jnp.concatenate(
            [
                jnp.broadcast_to(part[:, pair : pair + 1], (rows, DH)),
                jnp.broadcast_to(part[:, pairs + pair : pairs + pair + 1], (rows, DH)),
            ],
            axis=0,
        )

    def level_of(box, step):
        raw = box[step, :, span:].astype(jnp.float32)
        full = raw + pltpu.roll(raw, DH - columns, 1) + pltpu.roll(raw, DH - 2 * columns, 1)
        return jnp.where(tag < columns, full, NEG)

    def packed(level):
        high = level.astype(jnp.bfloat16).astype(jnp.float32)
        rest = level - high
        middle = rest.astype(jnp.bfloat16).astype(jnp.float32)
        low = rest - middle
        level = jnp.where(tag < columns, high, jnp.where(tag < 2 * columns, middle, low))
        return level.astype(jnp.bfloat16)

    def merge(step):
        first, second = level_of(outbox, 2 * step + 1), level_of(sidebox, step)
        top = jnp.maximum(first, second)
        share, other = jnp.exp(first - top), jnp.exp(second - top)
        total = share + other
        inverse = 1.0 / total
        share, other = share * inverse, other * inverse
        for h in range(2 * pairs):
            piece = slice(h * DH, (h + 1) * DH)
            part = outbox[2 * step + 1, :, piece].astype(jnp.float32) * spread(share, h)
            part = part + sidebox[step, :, piece].astype(jnp.float32) * spread(other, h)
            merged[step, :, piece] = part.astype(jnp.bfloat16)
        level = top + jnp.log(total)
        level = jnp.where(tag < columns, level, 0.0)
        level = (
            level
            + jnp.where(tag < 2 * columns, pltpu.roll(level, columns, 1), 0.0)
            + pltpu.roll(level, 2 * columns, 1)
        )
        merged[step, :, span:] = packed(level)

    def block(step, fill):
        for j in range(2):
            for copy in streams(2 * step + j):
                copy.wait()
        if fill:
            for j in range(2):
                for copy in streams(2 * (step + ahead) + j):
                    copy.start()
        compute_both(2 * step)
        handover(step).start()

    def pass_on(step):
        handover(step).wait_recv()
        merge(step)
        message(step).start()

    pl.semaphore_wait(barrier, chips)
    block(0, ahead < chips)

    def turn(fill, step, carry):
        block(step, fill)
        pass_on(step - 1)
        return carry

    lax.fori_loop(1, chips - ahead, functools.partial(turn, True), 0)
    lax.fori_loop(max(1, chips - ahead), chips, functools.partial(turn, False), 0)

    small[2].wait()
    small[3].wait()
    query_own = squery[:, own].astype(jnp.float32)
    product = query_own * nkey[...].astype(jnp.float32)
    level_own = jnp.full((2 * rows, DH), NEG, jnp.float32)
    for pair in range(pairs):
        halves = [
            jnp.sum(product[:, h * DH : (h + 1) * DH], axis=1, keepdims=True) * (DH ** (-0.5))
            for h in (2 * pair, 2 * pair + 1)
        ]
        level_own = jnp.where(tag == pair, jnp.concatenate(halves, axis=0), level_own)

    boxes = [(outbox, parts - 1)] + [(inbox, step) for step in range(chips - 2)]
    boxes += [(sidebox, chips - 1), (inbox, chips - 2)]
    top = level_own
    for k, (box, step) in enumerate(boxes):
        if box is inbox:
            message(step).wait_recv()
        if box is sidebox:
            handover(step).wait_recv()
        level = level_of(box, step)
        stats[k] = level
        top = jnp.maximum(top, level)
    share = jnp.exp(level_own - top)
    total = share
    zero = jnp.zeros((rows, DH), jnp.float32)
    sums = [
        jnp.concatenate([nvalue[:, h * DH : (h + 1) * DH].astype(jnp.float32), zero], axis=0)
        * spread(share, h)
        for h in range(2 * pairs)
    ]
    for k, (box, step) in enumerate(boxes):
        share = jnp.exp(stats[k] - top)
        total = total + share
        for h in range(2 * pairs):
            part = box[step, :, h * DH : (h + 1) * DH].astype(jnp.float32)
            sums[h] = sums[h] + part * spread(share, h)
    inverse = 1.0 / total
    for h in range(2 * pairs):
        result = sums[h] * spread(inverse, h)
        out[:, h * DH : (h + 1) * DH] = result.astype(jnp.bfloat16)

    def drain(step, carry):
        message(step).wait_send()
        return carry

    lax.fori_loop(0, chips - 1, drain, 0)

    def drain_side(step, carry):
        handover(step).wait_send()
        return carry

    lax.fori_loop(0, chips, drain_side, 0)


def on_device(
    self_query,
    new_key,
    new_value,
    cache_keys,
    cache_values,
    lengths,
    db_keys,
    db_values,
    cross_query,
    neighbour_ids,
):
    parts = lax.axis_size("seq")
    rows, positions, width = cache_keys.shape
    entries, tokens, _ = db_keys.shape
    span = width // parts
    chips = parts // 2
    ahead = min(3, chips)
    half = jnp.bfloat16
    anywhere = pl.BlockSpec(memory_space=pl.ANY)
    vmem = pl.BlockSpec(memory_space=pltpu.VMEM)
    out = pl.pallas_call(
        functools.partial(kernel, parts, ahead),
        out_shape=jax.ShapeDtypeStruct((2 * rows, span), half),
        in_specs=[anywhere] * 10,
        out_specs=vmem,
        scratch_shapes=[
            pltpu.SMEM(lengths.shape, jnp.int32),
            pltpu.SMEM(neighbour_ids.shape[::-1], jnp.int32),
            pltpu.VMEM((parts, rows, positions, span), half),
            pltpu.VMEM((parts, rows, positions, span), half),
            pltpu.VMEM((parts, entries, tokens, span), half),
            pltpu.VMEM((parts, entries, tokens, span), half),
            pltpu.VMEM((rows, width), half),
            pltpu.VMEM((rows, width), half),
            pltpu.VMEM((rows, span), half),
            pltpu.VMEM((rows, span), half),
            pltpu.VMEM((2 * rows, rows * positions), jnp.float32),
            pltpu.VMEM((2 * rows, entries * tokens), jnp.float32),
            pltpu.VMEM((2 * rows, entries * tokens), jnp.float32),
            pltpu.VMEM((parts, 2 * rows, span + DH), half),
            pltpu.VMEM((chips, 2 * rows, span + DH), half),
            pltpu.VMEM((chips, 2 * rows, span + DH), half),
            pltpu.VMEM((chips, 2 * rows, span + DH), half),
            pltpu.VMEM((chips + 1, 2 * rows, DH), jnp.float32),
            pltpu.SemaphoreType.DMA((4, parts)),
            pltpu.SemaphoreType.DMA((6,)),
            pltpu.SemaphoreType.DMA((chips,)),
            pltpu.SemaphoreType.DMA((chips,)),
            pltpu.SemaphoreType.DMA((chips,)),
            pltpu.SemaphoreType.DMA((chips,)),
        ],
        compiler_params=pltpu.CompilerParams(
            collective_id=0, has_side_effects=True, vmem_limit_bytes=60 * 1024 * 1024
        ),
    )(
        lengths,
        neighbour_ids.T,
        self_query,
        new_key,
        new_value,
        cache_keys,
        cache_values,
        db_keys,
        db_values,
        cross_query,
    )
    return out[:rows], out[rows:]


def solution(mesh):
    in_specs = (
        P("groups", None),
        P("groups", None),
        P("groups", None),
        P("groups", "seq", None),
        P("groups", "seq", None),
        P("groups"),
        P(("groups", "seq"), None, None),
        P(("groups", "seq"), None, None),
        P("groups", None),
        P("groups", None),
    )
    out_specs = (P("groups", "seq"), P("groups", "seq"))
    return jax.shard_map(
        on_device, mesh=mesh, in_specs=in_specs, out_specs=out_specs, check_vma=False
    )
```
